32 devices in a mesh: slab: 4 (over z), swap: 8 (over y, x, core).
Axes of the slice: x: 2, y: 2, z: 4, core: 2. Of those that a mesh axis runs over, the one named last changes fastest.
Arguments:
- fluid_state: float32 [2, 128, 128, 256], P(None, ('slab', 'swap')), may hold values from -0.45 to 1.6, as said below
- material: int32 [128, 128, 256], P(('slab', 'swap')), may hold values from 0 to 7
- table_colour: float32 [3, 8], replicated, may hold values from 0.2 to 2
- table_extinction: float32 [8], replicated, may hold values from 0.2 to 1.5
Outputs:
- new_density: float32 [128, 128, 256], P(('slab', 'swap'))
- rendered: float32 [4, 32768], P(None, 'swap')
The draws below stay inside these ranges and needn't reach their ends.
Inputs may be any that keep to these rules, and one draw needn't show every extreme that they name: fluid_state[0] is the density, between 0.6 and 1.6; fluid_state[1] is the momentum along the view axis, between -0.45 and 0.45.
All inputs are finite; a program needn't handle non-finite values.
Results may differ from the reference program's by a relative error of at most 0.0003.
Values sent between devices are 32-bit elements; how exact they have to be, the bound alone decides.
A program may use at most 64 MiB of HBM per device.

```python
import math
import jax
import jax.numpy as jnp

NX = 128
NY = 256
MATERIALS = 8
NZ = 128


def draw_fluid_state(key, part):
    first_key, second_key = jax.random.split(jax.random.fold_in(key, 11))
    extent = (NZ, NX, NY)
    density = jnp.exp(jax.random.uniform(first_key, extent, jnp.float32, math.log(0.6), math.log(1.6)))
    momentum = jax.random.uniform(second_key, extent, jnp.float32, -0.45, 0.45)
    return jnp.stack([density, momentum]).astype(jnp.float32)


def place_ends(array, key, low, top_value):
    shape = array.shape
    place = [jax.random.randint(jax.random.fold_in(key, axis), (), 0, shape[axis]) for axis in range(len(shape))]
    array = array.at[tuple(place)].set(low)
    longest = shape.index(max(shape))
    place[longest] = (place[longest] + 1) % shape[longest]
    return array.at[tuple(place)].set(top_value)


def setup_inputs(seed: int = 0) -> dict:
    splits = jax.random.split(jax.random.key(seed), 5)
    return {
        "fluid_state": draw_fluid_state(jax.random.fold_in(splits[4], 71), 0),
        "material": place_ends(jax.random.randint(splits[1], (NZ, NX, NY), 0, MATERIALS), jax.random.fold_in(splits[1], 1), 0, MATERIALS - 1).astype(jnp.int32),
        "table_colour": jnp.clip(jax.random.uniform(splits[2], (3, MATERIALS), jnp.float32, 0.2, 2.0), 0.2, 2.0),
        "table_extinction": jnp.clip(jnp.exp(jax.random.uniform(splits[3], (MATERIALS,), jnp.float32, math.log(0.2), math.log(1.5))), 0.2, 1.5),
    }


COURANT = 0.4
DEPTH_SCALE = 2.5


def hydro_step(fields):
    density = fields[0]
    momentum = fields[1]
    velocity = momentum / density
    speeds = jnp.abs(velocity) + 1.0
    fluxes = jnp.stack([momentum, momentum * velocity + density])
    face_speed = jnp.maximum(speeds[:-1], speeds[1:])
    face_flux = 0.5 * (fluxes[:, :-1] + fluxes[:, 1:]) - 0.5 * face_speed * (fields[:, 1:] - fields[:, :-1])
    return fields[:, 1:-1] - COURANT * (face_flux[:, 1:] - face_flux[:, :-1])


def reference(fluid_state, material, table_colour, table_extinction):
    fields = fluid_state
    for number in range(4):
        padded = jnp.concatenate([fields[:, -1:], fields, fields[:, :1]], axis=1)
        fields = hydro_step(padded)
    density = fields[0]
    extinction = jnp.zeros(density.shape, jnp.float32)
    for number in range(MATERIALS):
        extinction = extinction + jnp.where(material == number, table_extinction[number], 0.0)
    optical = DEPTH_SCALE * extinction * density / NZ
    running = jnp.cumsum(optical, axis=0)
    weight = jnp.exp(optical - running) * (1.0 - jnp.exp(-optical))
    colour = jnp.zeros((3, NX, NY), jnp.float32)
    for number in range(MATERIALS):
        summed = jnp.sum(jnp.where(material == number, weight, 0.0), axis=0)
        colour = colour + table_colour[:, number][:, None, None] * summed[None]
    opacity = 1.0 - jnp.exp(-running[-1])
    rendered = jnp.concatenate([colour, opacity[None]], axis=0).reshape(4, NX * NY)
    return density, rendered
```

```python
import functools

import jax
import jax.numpy as jnp
from jax import lax
from jax.experimental import pallas as pl
from jax.experimental.pallas import tpu as pltpu
from jax.sharding import PartitionSpec as P

COURANT = 0.4
DEPTH_SCALE = 2.5
STEPS = 4
VMEM_BYTES = 67043328
SPARE = 128 * 1024
MESH = pl.DeviceIdType.MESH


def largest_divisor(number, limit):
    return max(d for d in range(1, limit + 1) if number % d == 0)


def advance(state, density, momentum):
    velocity = momentum / density
    speed = jnp.abs(velocity) + 1.0
    flux = momentum * velocity + density
    if state is None:
        return (density, momentum, flux, speed, None, None), None
    old_density, old_momentum, old_flux, old_speed, old_face_d, old_face_m = state
    face_speed = jnp.maximum(old_speed, speed)
    face_d = (old_momentum + momentum) - face_speed * (density - old_density)
    face_m = (old_flux + flux) - face_speed * (momentum - old_momentum)
    state = (density, momentum, flux, speed, face_d, face_m)
    if old_face_d is None:
        return state, None
    half = 0.5 * COURANT
    new_density = old_density - half * (face_d - old_face_d)
    new_momentum = old_momentum - half * (face_m - old_face_m)
    return state, (new_density, new_momentum)


def lookup(masks, values):
    for mask in masks:
        values = [
            jnp.where(mask, values[i + 1], values[i]) if i + 1 < len(values) else values[i]
            for i in range(0, len(values), 2)
        ]
    return values[0]


def kernel(
    dims,
    fields,
    material,
    colour_source,
    extinction_source,
    out_density,
    out_image,
    staged,
    staged_material,
    held,
    held_material,
    new_density,
    pieces,
    image,
    colour_table,
    extinction_table,
    table_sem,
    image_sem,
    load_sem,
    load_material_sem,
    send_sem,
    field_sem,
    halo_sem,
    material_sem,
    back_sem,
    piece_sem,
    plane_sem,
    ready_sem,
    go_sem,
):
    slabs, members, depth, rows, cols, chunk_rows, chunk_cols = dims
    slab = lax.axis_index("slab")
    me = lax.axis_index("swap")
    gate = 1
    layers = members * depth
    width = STEPS
    across = cols // chunk_cols
    chunks = (rows // chunk_rows) * across
    materials = extinction_table.shape[0]

    def spot(c):
        return (
            pl.ds(pl.multiple_of(c // across * chunk_rows, chunk_rows), chunk_rows),
            pl.ds(pl.multiple_of(c % across * chunk_cols, chunk_cols), chunk_cols),
        )

    loads = []
    material_loads = []
    mine = pl.ds(width + me * depth, depth)
    mine_material = pl.ds(me * depth, depth)
    for c in range(chunks):
        r, l = spot(c)
        loads.append(
            pltpu.make_async_copy(
                fields.at[:, :, :, r, l], staged.at[:, :, :, r, l], load_sem.at[c]
            )
        )
        loads[-1].start()
    for c in range(chunks):
        r, l = spot(c)
        material_loads.append(
            pltpu.make_async_copy(
                material.at[:, :, r, l],
                staged_material.at[:, :, r, l],
                load_material_sem.at[c],
            )
        )
        material_loads[-1].start()

    tables = (
        pltpu.make_async_copy(colour_source, colour_table, table_sem.at[0]),
        pltpu.make_async_copy(extinction_source, extinction_table, table_sem.at[1]),
    )
    for table in tables:
        table.start()

    barrier = pltpu.get_barrier_semaphore()
    behind = lax.rem(slab + slabs - 1, slabs)
    ahead = lax.rem(slab + 1, slabs)
    def to_other_slabs(sem):
        @pl.loop(1, slabs)
        def _(k):
            pl.semaphore_signal(
                sem, inc=1, device_id=(lax.rem(slab + k, slabs), me), device_id_type=MESH
            )

    def to_plane(sem):
        @pl.loop(1, members)
        def _(k):
            other = lax.rem(me + k, members)

            @pl.when(other != gate)
            def _():
                pl.semaphore_signal(sem, inc=1, device_id=(slab, other), device_id_type=MESH)

    to_plane(barrier)

    @pl.when(me == gate)
    def _():
        to_other_slabs(barrier)

    @pl.when(me != gate)
    def _():
        pl.semaphore_wait(barrier, members - 1)
        pl.semaphore_signal(plane_sem, inc=1, device_id=(slab, gate), device_id_type=MESH)

    @pl.when(me == gate)
    def _():
        pl.semaphore_wait(plane_sem, members - 1)

    def send_fields(c):
        r, l = spot(c)
        @pl.loop(1, members)
        def _(k):
            other = lax.rem(me + k, members)
            pltpu.make_async_remote_copy(
                src_ref=staged.at[:, :, other, r, l],
                dst_ref=held.at[c, :, mine],
                send_sem=send_sem.at[0],
                recv_sem=field_sem.at[c, me],
                device_id=(slab, other),
                device_id_type=MESH,
            ).start()

    def send_material(c):
        r, l = spot(c)
        @pl.loop(1, members)
        def _(k):
            other = lax.rem(me + k, members)
            pltpu.make_async_remote_copy(
                src_ref=staged_material.at[:, other, r, l],
                dst_ref=held_material.at[c, mine_material],
                send_sem=send_sem.at[1],
                recv_sem=material_sem.at[c],
                device_id=(slab, other),
                device_id_type=MESH,
            ).start()

    for c in range(chunks):
        loads[c].wait()
        send_fields(c)
    for c in range(chunks):
        material_loads[c].wait()
        send_material(c)

    for c in range(chunks):
        r, l = spot(c)
        pltpu.make_async_copy(
            staged.at[:, :, me, r, l], held.at[c, :, mine], field_sem.at[c, me]
        ).start()
        pltpu.make_async_copy(
            staged_material.at[:, me, r, l], held_material.at[c, mine_material], material_sem.at[c]
        ).start()

    @pl.when(me == gate)
    def _():
        pl.semaphore_wait(barrier, slabs - 1)
        to_other_slabs(ready_sem)
        pl.semaphore_wait(ready_sem, slabs - 1)
        to_plane(go_sem)

    @pl.when(me != gate)
    def _():
        pl.semaphore_wait(go_sem, 1)

    def wait_for(ref, sem):
        pltpu.make_async_copy(ref, ref, sem).wait()

    def pass_halos(c):
        for side, (owner, start, target, to) in enumerate((
            (members - 1, layers, 0, ahead),
            (0, width, width + layers, behind),
        )):
            wait_for(held.at[c, :, pl.ds(width + owner * depth, depth)], field_sem.at[c, owner])
            pltpu.make_async_remote_copy(
                src_ref=held.at[c, :, pl.ds(start, width)],
                dst_ref=held.at[c, :, pl.ds(target, width)],
                send_sem=send_sem.at[2],
                recv_sem=halo_sem.at[c, side],
                device_id=(to, me),
                device_id_type=MESH,
            ).start()

    total = layers + 2 * width

    def sweep(c):
        states = [None] * STEPS
        for i in range(total):
            cell = held[c, 0, i], held[c, 1, i]
            for k in range(STEPS):
                states[k], cell = advance(states[k], *cell)
                if cell is None:
                    break
            if cell is not None:
                new_density[c, i - 2 * width] = cell[0]

    def send_back(c):
        r, l = spot(c)
        @pl.loop(1, members)
        def _(k):
            other = lax.rem(me + k, members)
            pltpu.make_async_remote_copy(
                src_ref=new_density.at[c, pl.ds(other * depth, depth)],
                dst_ref=out_density.at[:, me, r, l],
                send_sem=send_sem.at[3],
                recv_sem=back_sem,
                device_id=(slab, other),
                device_id_type=MESH,
            ).start()
        pltpu.make_async_copy(
            new_density.at[c, pl.ds(me * depth, depth)],
            out_density.at[:, me, r, l],
            back_sem,
        ).start()

    scale = DEPTH_SCALE / (slabs * layers)

    def render(c):
        wait_for(held_material.at[c], material_sem.at[c])
        zero = jnp.zeros((chunk_rows, chunk_cols), jnp.float32)
        rates = [extinction_table[n] * (-scale) for n in range(materials)]
        colours = [[colour_table[ch, n] for n in range(materials)] for ch in range(3)]

        through, sums = zero + 1.0, (zero,) * 3
        for i in range(layers):
            row = held_material[c, i]
            masks = [(row & (1 << bit)) != 0 for bit in range((materials - 1).bit_length())]
            rate = lookup(masks, rates)
            kept = jnp.exp(rate * new_density[c, i])
            weight = through * (1.0 - kept)
            sums = tuple(s + weight * lookup(masks, t) for s, t in zip(sums, colours))
            through = through * kept
        for ch in range(3):
            pieces[c, slab, ch] = sums[ch]
        pieces[c, slab, 3] = through

        @pl.loop(1, slabs)
        def _(k):
            pltpu.make_async_remote_copy(
                src_ref=pieces.at[c, slab],
                dst_ref=pieces.at[c, slab],
                send_sem=send_sem.at[4],
                recv_sem=piece_sem.at[c],
                device_id=(lax.rem(slab + k, slabs), me),
                device_id_type=MESH,
            ).start()

    pass_halos(0)
    for table in tables:
        table.wait()

    @pl.loop(0, chunks)
    def _(c):
        @pl.when(c + 1 < chunks)
        def _():
            pass_halos(c + 1)

        for m in range(1, members - 1):
            wait_for(held.at[c, :, pl.ds(width + m * depth, depth)], field_sem.at[c, m])
        for side in range(2):
            wait_for(held.at[c, :, pl.ds(0, width)], halo_sem.at[c, side])
        sweep(c)
        send_back(c)

        @pl.when(c > 0)
        def _():
            render(c - 1)

    render(chunks - 1)
    for c in range(chunks):
        wait_for(pieces.at[c, pl.ds(0, slabs - 1)], piece_sem.at[c])
        through = pieces[c, 0, 3]
        sums = [pieces[c, 0, ch] for ch in range(3)]
        for n in range(1, slabs):
            sums = [value + through * pieces[c, n, ch] for ch, value in enumerate(sums)]
            through = through * pieces[c, n, 3]
        for ch, value in enumerate(sums + [1.0 - through]):
            for q in range(chunk_rows):
                start = (c // across * chunk_rows + q) * cols + c % across * chunk_cols
                image[ch : ch + 1, start : start + chunk_cols] = value[q : q + 1]
    image_copy = pltpu.make_async_copy(image, out_image, image_sem)
    image_copy.start()

    others = pl.ds(0, members - 1)
    wait_for(staged.at[:, :, others], send_sem.at[0])
    wait_for(staged_material.at[:, others], send_sem.at[1])
    wait_for(held.at[:, :, pl.ds(0, 2 * width)], send_sem.at[2])
    wait_for(new_density.at[:, pl.ds(0, (members - 1) * depth)], send_sem.at[3])
    wait_for(pieces.at[:, pl.ds(0, slabs - 1)], send_sem.at[4])
    wait_for(out_density, back_sem)
    image_copy.wait()


def put_kernel(density, image, out_density, out_image, sems):
    copies = (
        pltpu.make_async_copy(density, out_density, sems.at[0]),
        pltpu.make_async_copy(image, out_image, sems.at[1]),
    )
    for copy in copies:
        copy.start()
    for copy in copies:
        copy.wait()


def write_out(density, image):
    return pl.pallas_call(
        put_kernel,
        out_shape=(
            jax.ShapeDtypeStruct(density.shape, density.dtype),
            jax.ShapeDtypeStruct(image.shape, image.dtype),
        ),
        in_specs=[pl.BlockSpec(memory_space=pl.ANY)] * 2,
        out_specs=(pl.BlockSpec(memory_space=pl.ANY),) * 2,
        scratch_shapes=[pltpu.SemaphoreType.DMA((2,))],
        compiler_params=pltpu.CompilerParams(vmem_limit_bytes=1024 * 1024),
    )(density, image)


def per_device(fluid_state, material, table_colour, table_extinction):
    slabs = lax.axis_size("slab")
    members = lax.axis_size("swap")
    _, depth, height, cols = fluid_state.shape
    rows = height // members
    chunk_rows = 8 if rows % 8 == 0 else rows
    chunk_cols = cols
    chunks = (rows // chunk_rows) * (cols // chunk_cols)
    layers = members * depth
    tile = (chunk_rows, chunk_cols)
    grant = VMEM_BYTES - 4 * rows * cols * (depth * members + 4) - SPARE
    dims = (slabs, members, depth, rows, cols, chunk_rows, chunk_cols)
    density, image = pl.pallas_call(
        functools.partial(kernel, dims),
        out_shape=(
            pltpu.VMEM((depth, members, rows, cols), jnp.float32),
            pltpu.VMEM((4, rows * cols), jnp.float32),
        ),
        in_specs=[
            pl.BlockSpec(memory_space=pltpu.HBM),
            pl.BlockSpec(memory_space=pltpu.HBM),
            pl.BlockSpec(memory_space=pltpu.HBM),
            pl.BlockSpec(memory_space=pltpu.HBM),
        ],
        out_specs=(
            pl.BlockSpec(memory_space=pl.ANY),
            pl.BlockSpec(memory_space=pl.ANY),
        ),
        scratch_shapes=[
            pltpu.VMEM((2, depth, members, rows, cols), jnp.float32),
            pltpu.VMEM((depth, members, rows, cols), jnp.int32),
            pltpu.VMEM((chunks, 2, layers + 2 * STEPS) + tile, jnp.float32),
            pltpu.VMEM((chunks, layers) + tile, jnp.int32),
            pltpu.VMEM((chunks, layers) + tile, jnp.float32),
            pltpu.VMEM((chunks, slabs, 4) + tile, jnp.float32),
            pltpu.VMEM((4, rows * cols), jnp.float32),
            pltpu.SMEM(table_colour.shape, jnp.float32),
            pltpu.SMEM(table_extinction.shape, jnp.float32),
            pltpu.SemaphoreType.DMA((2,)),
            pltpu.SemaphoreType.DMA,
            pltpu.SemaphoreType.DMA((chunks,)),
            pltpu.SemaphoreType.DMA((chunks,)),
            pltpu.SemaphoreType.DMA((5,)),
            pltpu.SemaphoreType.DMA((chunks, members)),
            pltpu.SemaphoreType.DMA((chunks, 2)),
            pltpu.SemaphoreType.DMA((chunks,)),
            pltpu.SemaphoreType.DMA,
            pltpu.SemaphoreType.DMA((chunks,)),
            pltpu.SemaphoreType.REGULAR,
            pltpu.SemaphoreType.REGULAR,
            pltpu.SemaphoreType.REGULAR,
        ],
        compiler_params=pltpu.CompilerParams(
            collective_id=0, has_side_effects=True, vmem_limit_bytes=grant
        ),
    )(
        fluid_state.reshape(2, depth, members, rows, cols),
        material.reshape(depth, members, rows, cols),
        table_colour,
        table_extinction,
    )
    return write_out(density.reshape(depth, height, cols), image)


def solution(mesh):
    return jax.shard_map(
        per_device,
        mesh=mesh,
        in_specs=(P(None, ("slab", "swap"), None, None), P(("slab", "swap"), None, None), P(), P()),
        out_specs=(P(("slab", "swap"), None, None), P(None, "swap")),
        check_vma=False,
    )
```

```python
import functools

import jax
import jax.numpy as jnp
from jax import lax
from jax.experimental import pallas as pl
from jax.experimental.pallas import tpu as pltpu
from jax.sharding import PartitionSpec as P

COURANT = 0.4
DEPTH_SCALE = 2.5
STEPS = 4
VMEM_BYTES = 67043328
SPARE = 128 * 1024
MESH = pl.DeviceIdType.MESH


def largest_divisor(number, limit):
    return max(d for d in range(1, limit + 1) if number % d == 0)


def advance(state, density, momentum):
    velocity = momentum / density
    speed = jnp.abs(velocity) + 1.0
    flux = momentum * velocity + density
    if state is None:
        return (density, momentum, flux, speed, None, None), None
    old_density, old_momentum, old_flux, old_speed, old_face_d, old_face_m = state
    face_speed = jnp.maximum(old_speed, speed)
    face_d = (old_momentum + momentum) - face_speed * (density - old_density)
    face_m = (old_flux + flux) - face_speed * (momentum - old_momentum)
    state = (density, momentum, flux, speed, face_d, face_m)
    if old_face_d is None:
        return state, None
    half = 0.5 * COURANT
    new_density = old_density - half * (face_d - old_face_d)
    new_momentum = old_momentum - half * (face_m - old_face_m)
    return state, (new_density, new_momentum)


def lookup(masks, values):
    for mask in masks:
        values = [
            jnp.where(mask, values[i + 1], values[i]) if i + 1 < len(values) else values[i]
            for i in range(0, len(values), 2)
        ]
    return values[0]


def kernel(
    dims,
    fields,
    material,
    colour_source,
    extinction_source,
    out_density,
    out_image,
    staged,
    staged_material,
    held,
    held_material,
    new_density,
    pieces,
    image,
    colour_table,
    extinction_table,
    table_sem,
    image_sem,
    load_sem,
    load_material_sem,
    send_sem,
    field_sem,
    halo_sem,
    material_sem,
    back_sem,
    piece_sem,
    near_sem,
    all_sem,
    slab_sem,
):
    slabs, members, depth, rows, cols, chunk_rows, chunk_cols = dims
    slab = lax.axis_index("slab")
    me = lax.axis_index("swap")
    head, tail = 2, members - 2

    def each(low, high, skip=None):
        def run(body):
            def visit(m):
                wanted = m != me
                if skip is not None:
                    wanted = jnp.logical_and(wanted, m != skip)
                pl.when(wanted)(lambda: body(m))

            for core in range(2):
                if high - low <= 8:
                    for m in range(low + core, high, 2):
                        visit(m)
                else:
                    pl.loop(0, (high - low) // 2)(lambda k, core=core: visit(low + 2 * k + core))

        return run

    layers = members * depth
    width = STEPS
    across = cols // chunk_cols
    chunks = (rows // chunk_rows) * across
    materials = extinction_table.shape[0]

    def spot(c):
        return (
            pl.ds(pl.multiple_of(c // across * chunk_rows, chunk_rows), chunk_rows),
            pl.ds(pl.multiple_of(c % across * chunk_cols, chunk_cols), chunk_cols),
        )

    loads = []
    material_loads = []
    mine = pl.ds(width + me * depth, depth)
    mine_material = pl.ds(me * depth, depth)
    for c in range(chunks):
        r, l = spot(c)
        loads.append(
            pltpu.make_async_copy(
                fields.at[:, :, :, r, l], staged.at[:, :, :, r, l], load_sem.at[c]
            )
        )
        loads[-1].start()
    for c in range(chunks):
        r, l = spot(c)
        material_loads.append(
            pltpu.make_async_copy(
                material.at[:, :, r, l],
                staged_material.at[:, :, r, l],
                load_material_sem.at[c],
            )
        )
        material_loads[-1].start()

    tables = (
        pltpu.make_async_copy(colour_source, colour_table, table_sem.at[0]),
        pltpu.make_async_copy(extinction_source, extinction_table, table_sem.at[1]),
    )
    for table in tables:
        table.start()

    barrier = pltpu.get_barrier_semaphore()
    behind = lax.rem(slab + slabs - 1, slabs)
    ahead = lax.rem(slab + 1, slabs)
    early = me < head
    late = me >= tail
    paired = lax.rem(me, 2) == 1

    def to_range(sem, low, high):
        @pl.loop(low, high)
        def _(m):
            pl.semaphore_signal(sem, inc=1, device_id=(slab, m), device_id_type=MESH)

    def to_slabs(sem, low, high):
        @pl.loop(low, high)
        def _(n):
            pl.semaphore_signal(sem, inc=1, device_id=(n, me), device_id_type=MESH)

    @pl.when(jnp.logical_not(paired))
    def _():
        to_range(barrier, me + 1, me + 2)

    @pl.when(early)
    def _():
        to_range(barrier, head, members)

    @pl.when(jnp.logical_and(me >= head, me < tail))
    def _():
        to_range(barrier, tail, members)

    to_slabs(barrier, slab + 1, slabs)
    def wait_count(sem, count):
        @pl.when(count > 0)
        def _():
            pl.semaphore_wait(sem, count)

    wait_count(
        barrier,
        jnp.where(early, 0, jnp.where(late, tail, head)) + jnp.where(paired, 1, 0) + slab,
    )

    @pl.when(paired)
    def _():
        to_range(near_sem, me - 1, me)

    @pl.when(late)
    def _():
        to_range(all_sem, 0, tail)

    @pl.when(jnp.logical_and(me >= head, me < tail))
    def _():
        to_range(near_sem, 0, head)

    to_slabs(slab_sem, 0, slab)
    wait_count(near_sem, jnp.where(early, tail - head, 0) + jnp.where(paired, 0, 1))

    def field_copy(c, other):
        r, l = spot(c)
        return pltpu.make_async_remote_copy(
            src_ref=staged.at[:, :, other, r, l],
            dst_ref=held.at[c, :, mine],
            send_sem=send_sem.at[0],
            recv_sem=field_sem.at[c, me],
            device_id=(slab, other),
            device_id_type=MESH,
        )

    def send_fields(c, low, high, skip=None):
        @each(low, high, skip)
        def _(other):
            field_copy(c, other).start()

    def send_material(c):
        r, l = spot(c)

        @each(0, members)
        def _(other):
            pltpu.make_async_remote_copy(
                src_ref=staged_material.at[:, other, r, l],
                dst_ref=held_material.at[c, mine_material],
                send_sem=send_sem.at[1],
                recv_sem=material_sem.at[c, me],
                device_id=(slab, other),
                device_id_type=MESH,
            ).start()

    loads[0].wait()

    @pl.when(early)
    def _():
        send_fields(0, 0, tail)
        pl.semaphore_wait(all_sem, members - tail)
        send_fields(0, tail, members)

    @pl.when(jnp.logical_and(me >= head, me < tail))
    def _():
        buddy = me + 1 - 2 * lax.rem(me, 2)
        send_fields(0, 0, head)
        field_copy(0, buddy).start()
        pl.semaphore_wait(all_sem, members - tail)
        send_fields(0, head, members, buddy)

    @pl.when(late)
    def _():
        send_fields(0, 0, members)

    for c in range(1, chunks):
        loads[c].wait()
        send_fields(c, 0, members)
    for c in range(chunks):
        material_loads[c].wait()
        send_material(c)

    for c in range(chunks):
        r, l = spot(c)
        pltpu.make_async_copy(
            staged.at[:, :, me, r, l], held.at[c, :, mine], field_sem.at[c, me]
        ).start()
        pltpu.make_async_copy(
            staged_material.at[:, me, r, l], held_material.at[c, mine_material], material_sem.at[c, me]
        ).start()

    wait_count(slab_sem, slabs - 1 - slab)

    def wait_for(ref, sem):
        pltpu.make_async_copy(ref, ref, sem).wait()

    def pass_halos(c):
        for side, (owner, start, target, to) in enumerate((
            (members - 1, layers, 0, ahead),
            (0, width, width + layers, behind),
        )):
            wait_for(held.at[c, :, pl.ds(width + owner * depth, depth)], field_sem.at[c, owner])
            pltpu.make_async_remote_copy(
                src_ref=held.at[c, :, pl.ds(start, width)],
                dst_ref=held.at[c, :, pl.ds(target, width)],
                send_sem=send_sem.at[2],
                recv_sem=halo_sem.at[c, side],
                device_id=(to, me),
                device_id_type=MESH,
            ).start()

    total = layers + 2 * width

    def sweep(c):
        states = [None] * STEPS
        for i in range(total):
            cell = held[c, 0, i], held[c, 1, i]
            for k in range(STEPS):
                states[k], cell = advance(states[k], *cell)
                if cell is None:
                    break
            if cell is not None:
                new_density[c, i - 2 * width] = cell[0]

    def send_back(c):
        r, l = spot(c)
        @each(0, members)
        def _(other):
            pltpu.make_async_remote_copy(
                src_ref=new_density.at[c, pl.ds(other * depth, depth)],
                dst_ref=out_density.at[:, me, r, l],
                send_sem=send_sem.at[3],
                recv_sem=back_sem,
                device_id=(slab, other),
                device_id_type=MESH,
            ).start()
        pltpu.make_async_copy(
            new_density.at[c, pl.ds(me * depth, depth)],
            out_density.at[:, me, r, l],
            back_sem,
        ).start()

    scale = DEPTH_SCALE / (slabs * layers)

    def render(c):
        zero = jnp.zeros((chunk_rows, chunk_cols), jnp.float32)
        rates = [extinction_table[n] * (-scale) for n in range(materials)]
        colours = [[colour_table[ch, n] for n in range(materials)] for ch in range(3)]

        through, sums = zero + 1.0, (zero,) * 3
        for i in range(layers):
            if i % depth == 0:
                wait_for(held_material.at[c, pl.ds(i, depth)], material_sem.at[c, i // depth])
            row = held_material[c, i]
            masks = [(row & (1 << bit)) != 0 for bit in range((materials - 1).bit_length())]
            rate = lookup(masks, rates)
            kept = jnp.exp(rate * new_density[c, i])
            weight = through * (1.0 - kept)
            sums = tuple(s + weight * lookup(masks, t) for s, t in zip(sums, colours))
            through = through * kept
        for ch in range(3):
            pieces[c, slab, ch] = sums[ch]
        pieces[c, slab, 3] = through

        @pl.loop(1, slabs)
        def _(k):
            pltpu.make_async_remote_copy(
                src_ref=pieces.at[c, slab],
                dst_ref=pieces.at[c, slab],
                send_sem=send_sem.at[4],
                recv_sem=piece_sem.at[c],
                device_id=(lax.rem(slab + k, slabs), me),
                device_id_type=MESH,
            ).start()

    pass_halos(0)
    for table in tables:
        table.wait()

    @pl.loop(0, chunks)
    def _(c):
        @pl.when(c + 1 < chunks)
        def _():
            pass_halos(c + 1)

        for m in range(1, members - 1):
            wait_for(held.at[c, :, pl.ds(width + m * depth, depth)], field_sem.at[c, m])
        for side in range(2):
            wait_for(held.at[c, :, pl.ds(0, width)], halo_sem.at[c, side])
        sweep(c)
        send_back(c)

        @pl.when(c > 0)
        def _():
            render(c - 1)

    render(chunks - 1)
    for c in range(chunks):
        wait_for(pieces.at[c, pl.ds(0, slabs - 1)], piece_sem.at[c])
        through = pieces[c, 0, 3]
        sums = [pieces[c, 0, ch] for ch in range(3)]
        for n in range(1, slabs):
            sums = [value + through * pieces[c, n, ch] for ch, value in enumerate(sums)]
            through = through * pieces[c, n, 3]
        for ch, value in enumerate(sums + [1.0 - through]):
            for q in range(chunk_rows):
                start = (c // across * chunk_rows + q) * cols + c % across * chunk_cols
                image[ch : ch + 1, start : start + chunk_cols] = value[q : q + 1]
    image_copy = pltpu.make_async_copy(image, out_image, image_sem)
    image_copy.start()

    others = pl.ds(0, members - 1)
    wait_for(staged.at[:, :, others], send_sem.at[0])
    wait_for(staged_material.at[:, others], send_sem.at[1])
    wait_for(held.at[:, :, pl.ds(0, 2 * width)], send_sem.at[2])
    wait_for(new_density.at[:, pl.ds(0, (members - 1) * depth)], send_sem.at[3])
    wait_for(pieces.at[:, pl.ds(0, slabs - 1)], send_sem.at[4])
    wait_for(out_density, back_sem)
    image_copy.wait()


def put_kernel(density, image, out_density, out_image, sems):
    copies = (
        pltpu.make_async_copy(density, out_density, sems.at[0]),
        pltpu.make_async_copy(image, out_image, sems.at[1]),
    )
    for copy in copies:
        copy.start()
    for copy in copies:
        copy.wait()


def write_out(density, image):
    return pl.pallas_call(
        put_kernel,
        out_shape=(
            jax.ShapeDtypeStruct(density.shape, density.dtype),
            jax.ShapeDtypeStruct(image.shape, image.dtype),
        ),
        in_specs=[pl.BlockSpec(memory_space=pl.ANY)] * 2,
        out_specs=(pl.BlockSpec(memory_space=pl.ANY),) * 2,
        scratch_shapes=[pltpu.SemaphoreType.DMA((2,))],
        compiler_params=pltpu.CompilerParams(vmem_limit_bytes=1024 * 1024),
    )(density, image)


def per_device(fluid_state, material, table_colour, table_extinction):
    slabs = lax.axis_size("slab")
    members = lax.axis_size("swap")
    _, depth, height, cols = fluid_state.shape
    rows = height // members
    chunk_rows = 8 if rows % 8 == 0 else rows
    chunk_cols = cols
    chunks = (rows // chunk_rows) * (cols // chunk_cols)
    layers = members * depth
    tile = (chunk_rows, chunk_cols)
    grant = VMEM_BYTES - 4 * rows * cols * (depth * members + 4) - SPARE
    dims = (slabs, members, depth, rows, cols, chunk_rows, chunk_cols)
    density, image = pl.pallas_call(
        functools.partial(kernel, dims),
        out_shape=(
            pltpu.VMEM((depth, members, rows, cols), jnp.float32),
            pltpu.VMEM((4, rows * cols), jnp.float32),
        ),
        in_specs=[
            pl.BlockSpec(memory_space=pltpu.HBM),
            pl.BlockSpec(memory_space=pltpu.HBM),
            pl.BlockSpec(memory_space=pltpu.HBM),
            pl.BlockSpec(memory_space=pltpu.HBM),
        ],
        out_specs=(
            pl.BlockSpec(memory_space=pl.ANY),
            pl.BlockSpec(memory_space=pl.ANY),
        ),
        scratch_shapes=[
            pltpu.VMEM((2, depth, members, rows, cols), jnp.float32),
            pltpu.VMEM((depth, members, rows, cols), jnp.int32),
            pltpu.VMEM((chunks, 2, layers + 2 * STEPS) + tile, jnp.float32),
            pltpu.VMEM((chunks, layers) + tile, jnp.int32),
            pltpu.VMEM((chunks, layers) + tile, jnp.float32),
            pltpu.VMEM((chunks, slabs, 4) + tile, jnp.float32),
            pltpu.VMEM((4, rows * cols), jnp.float32),
            pltpu.SMEM(table_colour.shape, jnp.float32),
            pltpu.SMEM(table_extinction.shape, jnp.float32),
            pltpu.SemaphoreType.DMA((2,)),
            pltpu.SemaphoreType.DMA,
            pltpu.SemaphoreType.DMA((chunks,)),
            pltpu.SemaphoreType.DMA((chunks,)),
            pltpu.SemaphoreType.DMA((5,)),
            pltpu.SemaphoreType.DMA((chunks, members)),
            pltpu.SemaphoreType.DMA((chunks, 2)),
            pltpu.SemaphoreType.DMA((chunks, members)),
            pltpu.SemaphoreType.DMA,
            pltpu.SemaphoreType.DMA((chunks,)),
            pltpu.SemaphoreType.REGULAR,
            pltpu.SemaphoreType.REGULAR,
            pltpu.SemaphoreType.REGULAR,
        ],
        compiler_params=pltpu.CompilerParams(
            collective_id=0, has_side_effects=True, vmem_limit_bytes=grant
        ),
    )(
        fluid_state.reshape(2, depth, members, rows, cols),
        material.reshape(depth, members, rows, cols),
        table_colour,
        table_extinction,
    )
    return write_out(density.reshape(depth, height, cols), image)


def solution(mesh):
    return jax.shard_map(
        per_device,
        mesh=mesh,
        in_specs=(P(None, ("slab", "swap"), None, None), P(("slab", "swap"), None, None), P(), P()),
        out_specs=(P(("slab", "swap"), None, None), P(None, "swap")),
        check_vma=False,
    )
```

```python
import functools

import jax
import jax.numpy as jnp
from jax import lax
from jax.experimental import pallas as pl
from jax.experimental.pallas import tpu as pltpu
from jax.sharding import PartitionSpec as P

COURANT = 0.4
DEPTH_SCALE = 2.5
STEPS = 4
VMEM_BYTES = 67043328
SPARE = 128 * 1024
MESH = pl.DeviceIdType.MESH


def largest_divisor(number, limit):
    return max(d for d in range(1, limit + 1) if number % d == 0)


def advance(state, density, momentum):
    velocity = momentum / density
    speed = jnp.abs(velocity) + 1.0
    flux = momentum * velocity + density
    if state is None:
        return (density, momentum, flux, speed, None, None), None
    old_density, old_momentum, old_flux, old_speed, old_face_d, old_face_m = state
    face_speed = jnp.maximum(old_speed, speed)
    face_d = (old_momentum + momentum) - face_speed * (density - old_density)
    face_m = (old_flux + flux) - face_speed * (momentum - old_momentum)
    state = (density, momentum, flux, speed, face_d, face_m)
    if old_face_d is None:
        return state, None
    half = 0.5 * COURANT
    new_density = old_density - half * (face_d - old_face_d)
    new_momentum = old_momentum - half * (face_m - old_face_m)
    return state, (new_density, new_momentum)


def lookup(masks, values):
    for mask in masks:
        values = [
            jnp.where(mask, values[i + 1], values[i]) if i + 1 < len(values) else values[i]
            for i in range(0, len(values), 2)
        ]
    return values[0]


def kernel(
    dims,
    fields,
    material,
    colour_source,
    extinction_source,
    out_density,
    out_image,
    staged,
    staged_material,
    held,
    held_material,
    new_density,
    pieces,
    rest,
    image,
    colour_table,
    extinction_table,
    table_sem,
    image_sem,
    load_sem,
    load_material_sem,
    send_sem,
    field_sem,
    halo_sem,
    material_sem,
    back_sem,
    piece_sem,
    near_sem,
    all_sem,
    slab_sem,
):
    slabs, members, depth, rows, cols, chunk_rows, chunk_cols = dims
    slab = lax.axis_index("slab")
    me = lax.axis_index("swap")
    head, tail = 2, members - 2

    def each(low, high, skip=None):
        def run(body):
            def visit(m):
                wanted = m != me
                if skip is not None:
                    wanted = jnp.logical_and(wanted, m != skip)
                pl.when(wanted)(lambda: body(m))

            for core in range(2):
                if high - low <= 8:
                    for m in range(low + core, high, 2):
                        visit(m)
                else:
                    pl.loop(0, (high - low) // 2)(lambda k, core=core: visit(low + 2 * k + core))

        return run

    layers = members * depth
    width = STEPS
    across = cols // chunk_cols
    chunks = (rows // chunk_rows) * across
    materials = extinction_table.shape[0]

    def spot(c):
        return (
            pl.ds(pl.multiple_of(c // across * chunk_rows, chunk_rows), chunk_rows),
            pl.ds(pl.multiple_of(c % across * chunk_cols, chunk_cols), chunk_cols),
        )

    loads = []
    material_loads = []
    mine = pl.ds(width + me * depth, depth)
    mine_material = pl.ds(me * depth, depth)
    for c in range(chunks):
        r, l = spot(c)
        loads.append(
            pltpu.make_async_copy(
                fields.at[:, :, :, r, l], staged.at[:, :, :, r, l], load_sem.at[c]
            )
        )
        loads[-1].start()
    for c in range(chunks):
        r, l = spot(c)
        material_loads.append(
            pltpu.make_async_copy(
                material.at[:, :, r, l],
                staged_material.at[:, :, r, l],
                load_material_sem.at[c],
            )
        )

    tables = (
        pltpu.make_async_copy(colour_source, colour_table, table_sem.at[0]),
        pltpu.make_async_copy(extinction_source, extinction_table, table_sem.at[1]),
    )
    for table in tables:
        table.start()

    barrier = pltpu.get_barrier_semaphore()
    behind = lax.rem(slab + slabs - 1, slabs)
    ahead = lax.rem(slab + 1, slabs)
    early = me < head
    late = me >= tail
    paired = lax.rem(me, 2) == 1

    def to_range(sem, low, high):
        @pl.loop(low, high)
        def _(m):
            pl.semaphore_signal(sem, inc=1, device_id=(slab, m), device_id_type=MESH)

    def to_slabs(sem, low, high):
        @pl.loop(low, high)
        def _(n):
            pl.semaphore_signal(sem, inc=1, device_id=(n, me), device_id_type=MESH)

    @pl.when(jnp.logical_not(paired))
    def _():
        to_range(barrier, me + 1, me + 2)

    @pl.when(early)
    def _():
        to_range(barrier, head, members)

    @pl.when(jnp.logical_and(me >= head, me < tail))
    def _():
        to_range(barrier, tail, members)

    to_slabs(barrier, slab + 1, slabs)
    def wait_count(sem, count):
        @pl.when(count > 0)
        def _():
            pl.semaphore_wait(sem, count)

    wait_count(
        barrier,
        jnp.where(early, 0, jnp.where(late, tail, head)) + jnp.where(paired, 1, 0) + slab,
    )

    @pl.when(paired)
    def _():
        to_range(near_sem, me - 1, me)

    @pl.when(late)
    def _():
        to_range(all_sem, 0, tail)

    @pl.when(jnp.logical_and(me >= head, me < tail))
    def _():
        to_range(near_sem, 0, head)

    to_slabs(slab_sem, 0, slab)
    wait_count(near_sem, jnp.where(early, tail - head, 0) + jnp.where(paired, 0, 1))

    def field_copy(c, other):
        r, l = spot(c)
        return pltpu.make_async_remote_copy(
            src_ref=staged.at[:, :, other, r, l],
            dst_ref=held.at[c, :, mine],
            send_sem=send_sem.at[0],
            recv_sem=field_sem.at[c, me],
            device_id=(slab, other),
            device_id_type=MESH,
        )

    def send_fields(c, low, high, skip=None):
        @each(low, high, skip)
        def _(other):
            field_copy(c, other).start()

    def send_material(c):
        r, l = spot(c)

        @each(0, members)
        def _(other):
            pltpu.make_async_remote_copy(
                src_ref=staged_material.at[:, other, r, l],
                dst_ref=held_material.at[c, mine_material],
                send_sem=send_sem.at[1],
                recv_sem=material_sem.at[c, me],
                device_id=(slab, other),
                device_id_type=MESH,
            ).start()

    loads[0].wait()
    for load in material_loads:
        load.start()

    @pl.when(early)
    def _():
        send_fields(0, 0, tail)
        pl.semaphore_wait(all_sem, members - tail)
        send_fields(0, tail, members)

    @pl.when(jnp.logical_and(me >= head, me < tail))
    def _():
        buddy = me + 1 - 2 * lax.rem(me, 2)
        send_fields(0, 0, head)
        field_copy(0, buddy).start()
        pl.semaphore_wait(all_sem, members - tail)
        send_fields(0, head, members, buddy)

    @pl.when(late)
    def _():
        send_fields(0, 0, members)

    for c in range(1, chunks):
        loads[c].wait()
        send_fields(c, 0, members)
    for c in range(chunks):
        material_loads[c].wait()
        send_material(c)

    for c in range(chunks):
        r, l = spot(c)
        pltpu.make_async_copy(
            staged.at[:, :, me, r, l], held.at[c, :, mine], field_sem.at[c, me]
        ).start()
        pltpu.make_async_copy(
            staged_material.at[:, me, r, l], held_material.at[c, mine_material], material_sem.at[c, me]
        ).start()

    wait_count(slab_sem, slabs - 1 - slab)

    def wait_for(ref, sem):
        pltpu.make_async_copy(ref, ref, sem).wait()

    def pass_halos(c):
        for side, (owner, start, target, to) in enumerate((
            (members - 1, layers, 0, ahead),
            (0, width, width + layers, behind),
        )):
            wait_for(held.at[c, :, pl.ds(width + owner * depth, depth)], field_sem.at[c, owner])
            pltpu.make_async_remote_copy(
                src_ref=held.at[c, :, pl.ds(start, width)],
                dst_ref=held.at[c, :, pl.ds(target, width)],
                send_sem=send_sem.at[2],
                recv_sem=halo_sem.at[c, side],
                device_id=(to, me),
                device_id_type=MESH,
            ).start()

    total = layers + 2 * width

    front = -(-width // depth)

    def stream(c, start, stop):
        states = [None] * STEPS
        for i in range(start, stop):
            cell = held[c, 0, i], held[c, 1, i]
            for k in range(STEPS):
                states[k], cell = advance(states[k], *cell)
                if cell is None:
                    break
            if cell is not None:
                new_density[c, i - 2 * width] = cell[0]

    def send_back(c):
        r = pl.ds(pl.multiple_of(c // across * chunk_rows, chunk_rows), chunk_rows)
        l = pl.ds(pl.multiple_of(c % across * chunk_cols, chunk_cols), chunk_cols)

        def send(other):
            pltpu.make_async_remote_copy(
                src_ref=new_density.at[c, pl.ds(other * depth, depth)],
                dst_ref=out_density.at[:, me, r, l],
                send_sem=send_sem.at[3],
                recv_sem=back_sem,
                device_id=(slab, other),
                device_id_type=MESH,
            ).start()

        each(0, members)(send)
        pltpu.make_async_copy(
            new_density.at[c, pl.ds(me * depth, depth)], out_density.at[:, me, r, l], back_sem
        ).start()

    def sweep_rest(c):
        for m in range(1, members - 1):
            wait_for(held.at[c, :, pl.ds(width + m * depth, depth)], field_sem.at[c, m])
        wait_for(held.at[c, :, pl.ds(0, width)], halo_sem.at[c, 1])
        stream(c, width, total)

    def sweep_front(c):
        wait_for(held.at[c, :, pl.ds(0, width)], halo_sem.at[c, 0])
        stream(c, 0, 3 * width)
        send_back(c)

    scale = DEPTH_SCALE / (slabs * layers)

    def absorb(c, low, high):
        zero = jnp.zeros((chunk_rows, chunk_cols), jnp.float32)
        rates = [extinction_table[n] * (-scale) for n in range(materials)]
        colours = [[colour_table[ch, n] for n in range(materials)] for ch in range(3)]
        through, sums = zero + 1.0, (zero,) * 3
        for i in range(low * depth, high * depth):
            if i % depth == 0:
                wait_for(held_material.at[c, pl.ds(i, depth)], material_sem.at[c, i // depth])
            row = held_material[c, i]
            masks = [(row & (1 << bit)) != 0 for bit in range((materials - 1).bit_length())]
            rate = lookup(masks, rates)
            kept = jnp.exp(rate * new_density[c, i])
            weight = through * (1.0 - kept)
            sums = tuple(s + weight * lookup(masks, t) for s, t in zip(sums, colours))
            through = through * kept
        return sums, through

    def render_rest(c):
        sums, through = absorb(c, front, members)
        for ch in range(3):
            rest[ch] = sums[ch]
        rest[3] = through

    def render_front(c):
        sums, through = absorb(c, 0, front)
        for ch in range(3):
            pieces[c, slab, ch] = sums[ch] + through * rest[ch]
        pieces[c, slab, 3] = through * rest[3]

        @pl.loop(1, slabs)
        def _(k):
            pltpu.make_async_remote_copy(
                src_ref=pieces.at[c, slab],
                dst_ref=pieces.at[c, slab],
                send_sem=send_sem.at[4],
                recv_sem=piece_sem.at[c],
                device_id=(lax.rem(slab + k, slabs), me),
                device_id_type=MESH,
            ).start()

    pass_halos(0)
    for table in tables:
        table.wait()

    end = chunks - 1

    @pl.loop(0, end)
    def _(c):
        pass_halos(c + 1)
        sweep_rest(c)
        sweep_front(c)

        @pl.when(c > 0)
        def _():
            render_rest(c - 1)
            render_front(c - 1)

    sweep_rest(end)
    if end > 0:
        render_rest(end - 1)
        render_front(end - 1)
    sweep_front(end)
    render_rest(end)
    render_front(end)

    for c in range(chunks):
        wait_for(pieces.at[c, pl.ds(0, slabs - 1)], piece_sem.at[c])
        through = pieces[c, 0, 3]
        sums = [pieces[c, 0, ch] for ch in range(3)]
        for n in range(1, slabs):
            sums = [value + through * pieces[c, n, ch] for ch, value in enumerate(sums)]
            through = through * pieces[c, n, 3]
        for ch, value in enumerate(sums + [1.0 - through]):
            for q in range(chunk_rows):
                start = (c // across * chunk_rows + q) * cols + c % across * chunk_cols
                image[ch : ch + 1, start : start + chunk_cols] = value[q : q + 1]
    image_copy = pltpu.make_async_copy(image, out_image, image_sem)
    image_copy.start()

    others = pl.ds(0, members - 1)
    wait_for(staged.at[:, :, others], send_sem.at[0])
    wait_for(staged_material.at[:, others], send_sem.at[1])
    wait_for(held.at[:, :, pl.ds(0, 2 * width)], send_sem.at[2])
    wait_for(new_density.at[:, pl.ds(0, (members - 1) * depth)], send_sem.at[3])
    wait_for(pieces.at[:, pl.ds(0, slabs - 1)], send_sem.at[4])
    wait_for(out_density, back_sem)
    image_copy.wait()


def put_kernel(density, image, out_density, out_image, sems):
    copies = (
        pltpu.make_async_copy(density, out_density, sems.at[0]),
        pltpu.make_async_copy(image, out_image, sems.at[1]),
    )
    for copy in copies:
        copy.start()
    for copy in copies:
        copy.wait()


def write_out(density, image):
    return pl.pallas_call(
        put_kernel,
        out_shape=(
            jax.ShapeDtypeStruct(density.shape, density.dtype),
            jax.ShapeDtypeStruct(image.shape, image.dtype),
        ),
        in_specs=[pl.BlockSpec(memory_space=pl.ANY)] * 2,
        out_specs=(pl.BlockSpec(memory_space=pl.ANY),) * 2,
        scratch_shapes=[pltpu.SemaphoreType.DMA((2,))],
        compiler_params=pltpu.CompilerParams(vmem_limit_bytes=1024 * 1024),
    )(density, image)


def per_device(fluid_state, material, table_colour, table_extinction):
    slabs = lax.axis_size("slab")
    members = lax.axis_size("swap")
    _, depth, height, cols = fluid_state.shape
    rows = height // members
    chunk_rows = 8 if rows % 8 == 0 else rows
    chunk_cols = cols
    chunks = (rows // chunk_rows) * (cols // chunk_cols)
    layers = members * depth
    tile = (chunk_rows, chunk_cols)
    grant = VMEM_BYTES - 4 * rows * cols * (depth * members + 4) - SPARE
    dims = (slabs, members, depth, rows, cols, chunk_rows, chunk_cols)
    density, image = pl.pallas_call(
        functools.partial(kernel, dims),
        out_shape=(
            pltpu.VMEM((depth, members, rows, cols), jnp.float32),
            pltpu.VMEM((4, rows * cols), jnp.float32),
        ),
        in_specs=[
            pl.BlockSpec(memory_space=pltpu.HBM),
            pl.BlockSpec(memory_space=pltpu.HBM),
            pl.BlockSpec(memory_space=pltpu.HBM),
            pl.BlockSpec(memory_space=pltpu.HBM),
        ],
        out_specs=(
            pl.BlockSpec(memory_space=pl.ANY),
            pl.BlockSpec(memory_space=pl.ANY),
        ),
        scratch_shapes=[
            pltpu.VMEM((2, depth, members, rows, cols), jnp.float32),
            pltpu.VMEM((depth, members, rows, cols), jnp.int32),
            pltpu.VMEM((chunks, 2, layers + 2 * STEPS) + tile, jnp.float32),
            pltpu.VMEM((chunks, layers) + tile, jnp.int32),
            pltpu.VMEM((chunks, layers) + tile, jnp.float32),
            pltpu.VMEM((chunks, slabs, 4) + tile, jnp.float32),
            pltpu.VMEM((4,) + tile, jnp.float32),
            pltpu.VMEM((4, rows * cols), jnp.float32),
            pltpu.SMEM(table_colour.shape, jnp.float32),
            pltpu.SMEM(table_extinction.shape, jnp.float32),
            pltpu.SemaphoreType.DMA((2,)),
            pltpu.SemaphoreType.DMA,
            pltpu.SemaphoreType.DMA((chunks,)),
            pltpu.SemaphoreType.DMA((chunks,)),
            pltpu.SemaphoreType.DMA((5,)),
            pltpu.SemaphoreType.DMA((chunks, members)),
            pltpu.SemaphoreType.DMA((chunks, 2)),
            pltpu.SemaphoreType.DMA((chunks, members)),
            pltpu.SemaphoreType.DMA,
            pltpu.SemaphoreType.DMA((chunks,)),
            pltpu.SemaphoreType.REGULAR,
            pltpu.SemaphoreType.REGULAR,
            pltpu.SemaphoreType.REGULAR,
        ],
        compiler_params=pltpu.CompilerParams(
            collective_id=0, has_side_effects=True, vmem_limit_bytes=grant
        ),
    )(
        fluid_state.reshape(2, depth, members, rows, cols),
        material.reshape(depth, members, rows, cols),
        table_colour,
        table_extinction,
    )
    return write_out(density.reshape(depth, height, cols), image)


def solution(mesh):
    return jax.shard_map(
        per_device,
        mesh=mesh,
        in_specs=(P(None, ("slab", "swap"), None, None), P(("slab", "swap"), None, None), P(), P()),
        out_specs=(P(("slab", "swap"), None, None), P(None, "swap")),
        check_vma=False,
    )
```
